8 devices in a mesh: dp: 1 (over z), sp: 8 (over x, y, core).
Axes of the slice: x: 2, y: 2, z: 1, core: 2. Of those that a mesh axis runs over, the one named last changes fastest.
Arguments:
- x: bfloat16 [2048, 6144], P(('dp', 'sp'))
- gain: bfloat16 [6144], replicated
- wq: bfloat16 [6144, 6144], replicated
- wk: bfloat16 [6144, 1024], replicated
- wv: bfloat16 [6144, 1024], replicated
- wo: bfloat16 [6144, 6144], replicated
Outputs:
- output: bfloat16 [2048, 6144], P(('dp', 'sp'))
All inputs are finite; a program needn't handle non-finite values.
Results may differ from the reference program's by a relative error of at most 0.012.
Values are sent between devices in bfloat16 or wider.
A program may use at most 2 GiB of HBM per device.

```python
import jax
import jax.numpy as jnp
from jax import lax

ROWS = 2048
D = 6144
HEADS = 48
KV_HEADS = 8
HEAD = 128
THETA = 10000


def setup_inputs(seed: int = 0, part: int = 0) -> dict:
    kx, kn, kq, kk, kv, ko = jax.random.split(jax.random.key(seed), 6)

    def weights(key, rows, columns):
        return jax.random.normal(key, (rows, columns), jnp.float32) * rows**-0.5

    drawn = {
        "x": jax.random.normal(jax.random.fold_in(kx, part), (ROWS, D), jnp.float32),
        "gain": 1 + 0.1 * jax.random.normal(kn, (D,), jnp.float32),
        "wq": 2 * weights(kq, D, HEADS * HEAD),
        "wk": 2 * weights(kk, D, KV_HEADS * HEAD),
        "wv": 4 * weights(kv, D, KV_HEADS * HEAD),
        "wo": weights(ko, HEADS * HEAD, D),
    }
    return {k: v.astype(jnp.bfloat16) for k, v in drawn.items()}


def normed(x, gain):
    wide = x.astype(jnp.float32)
    scale = lax.rsqrt(jnp.mean(wide * wide, -1, keepdims=True) + 1e-6)
    return (wide * scale * gain.astype(jnp.float32)).astype(jnp.bfloat16)


def turned(t, place, theta):
    half = t.shape[-1] // 2
    angle = place.astype(jnp.float32)[:, None] * theta ** (-jnp.arange(half, dtype=jnp.float32) / half)
    cos, sin = jnp.cos(angle)[:, None], jnp.sin(angle)[:, None]
    a, b = t[..., :half].astype(jnp.float32), t[..., half:].astype(jnp.float32)
    return jnp.concatenate([a * cos - b * sin, b * cos + a * sin], -1).astype(jnp.bfloat16)


def matmul(a, w):
    return jnp.dot(a, w, preferred_element_type=jnp.float32).astype(jnp.bfloat16)


def einsum(form, a, b):
    return jnp.einsum(form, a.astype(jnp.float32), b.astype(jnp.float32))


def attention(q, k, v):
    scores = einsum("tgsd,ugd->gstu", q, k) * q.shape[-1] ** -0.5
    token = jnp.arange(q.shape[0])
    scores = jnp.where(token[:, None] >= token, scores, -jnp.inf)
    weights = jax.nn.softmax(scores, -1).astype(jnp.bfloat16)
    return einsum("gstu,ugd->tgsd", weights, v).astype(jnp.bfloat16)


def reference(x, gain, wq, wk, wv, wo):
    a, place = normed(x, gain), jnp.arange(ROWS)
    q = turned(matmul(a, wq).reshape(ROWS, HEADS, HEAD), place, THETA).reshape(ROWS, KV_HEADS, -1, HEAD)
    k = turned(matmul(a, wk).reshape(ROWS, KV_HEADS, HEAD), place, THETA)
    v = matmul(a, wv).reshape(ROWS, KV_HEADS, HEAD)
    seen = attention(q, k, v).reshape(ROWS, HEADS * HEAD)
    return (x.astype(jnp.float32) + jnp.dot(seen, wo, preferred_element_type=jnp.float32)).astype(jnp.bfloat16)
```

```python
import functools

import jax
import jax.numpy as jnp
from jax import lax
from jax.experimental import pallas as pl
from jax.experimental.pallas import tpu as pltpu
from jax.sharding import PartitionSpec as P

HEAD = 128
THETA = 10000
LOG2E = 1.4426950408889634
HIDDEN = -1e30
MESH = pl.DeviceIdType.MESH
F32, BF16 = jnp.float32, jnp.bfloat16

D = 6144
OWN = 256
TOK = 512
CHIPS = 4
KV = 4
G = 6
NH = KV * G
HALF = D // 2
W = 512
SLOTS = 6
NQKV = 8
NOUT = D // W
SCALE2 = HEAD**-0.5 * LOG2E


def _dot(a, b, ca, cb):
    return lax.dot_general(a, b, (((ca,), (cb,)), ((), ())), preferred_element_type=F32)


def _kernel(x_ref, gain_ref, freq_ref, wq_ref, wk_ref, wv_ref, wo_ref, y_ref,
            x_own, x_part, wbuf, kv, q_all, o_all, yrecv, cos_s, sin_s,
            xsem, xs_sem, xr_sem, wsem, kvs, kvr, yss, yrs, osem):
    me = lax.axis_index("sp")
    chip, core = me // 2, me % 2
    partner = me + 1 - 2 * core

    barrier = pltpu.get_barrier_semaphore()
    for d in range(1, 8):
        pl.semaphore_signal(barrier, inc=1, device_id={"sp": (me + d) % 8}, device_id_type=MESH)

    def take(w_ref, row, col, slot):
        return pltpu.make_async_copy(w_ref.at[pl.ds(row, HALF), pl.ds(col, W)], wbuf.at[slot], wsem.at[slot])

    def take_full(w_ref, col, s):
        col = pl.multiple_of(col, W)
        take(w_ref, 0, col, 2 * s).start()
        take(w_ref, HALF, col, 2 * s + 1).start()

    def take_out(n, slot):
        return take(wo_ref, pl.multiple_of(core * HALF, HALF), pl.multiple_of(n * W, W), slot)

    x_in = pltpu.make_async_copy(x_ref, x_own, xsem)
    x_in.start()
    take_full(wk_ref, core * W, 0)
    take_full(wv_ref, core * W, 1)
    take_full(wq_ref, core * HALF, 2)

    pl.semaphore_wait(barrier, 7)
    x_swap = pltpu.make_async_remote_copy(src_ref=x_ref, dst_ref=x_part, send_sem=xs_sem, recv_sem=xr_sem,
                                          device_id={"sp": partner}, device_id_type=MESH)
    x_swap.start()

    place = (chip * TOK + lax.broadcasted_iota(jnp.int32, (TOK, HEAD), 0)).astype(F32)
    angle = place * freq_ref[...]
    cos_s[...] = jnp.cos(angle)
    sin_s[...] = jnp.where(lax.broadcasted_iota(jnp.int32, (TOK, HEAD), 1) < HEAD // 2, -1.0, 1.0) * jnp.sin(angle)

    def project(a_all, sc):
        def norm(src, base):
            def chunk(i, _):
                wide = src[pl.ds(pl.multiple_of(i * 32, 32), 32), :].astype(F32)
                scale = lax.rsqrt(jnp.mean(wide * wide, -1, keepdims=True) + 1e-6)
                a_all[pl.ds(pl.multiple_of(base + i * 32, 32), 32), :] = (wide * scale * gain_ref[...].astype(F32)).astype(BF16)
                return 0
            lax.fori_loop(0, OWN // 32, chunk, 0)

        x_in.wait()
        norm(x_own, core * OWN)
        x_swap.wait_recv()
        norm(x_part, (1 - core) * OWN)

        def turned(h):
            t = sc[:, h * HEAD : (h + 1) * HEAD].astype(BF16).astype(F32)
            return (t * cos_s[...] + pltpu.roll(t, HEAD // 2, 1) * sin_s[...]).astype(BF16)

        def block(j, _):
            s = lax.rem(j, 3)
            for i in range(2):
                take(wq_ref, 0, 0, 2 * s + i).wait()
            sc[...] = _dot(a_all[:, :HALF], wbuf[2 * s], 1, 0) + _dot(a_all[:, HALF:], wbuf[2 * s + 1], 1, 0)

            @pl.when(j + 3 < NQKV)
            def _():
                take_full(wq_ref, core * HALF + (j + 1) * W, s)

            @pl.when(j + 3 >= NQKV)
            def _():
                for i in range(2):
                    take_out(2 * (j + 3 - NQKV) + i, 2 * s + i).start()

            @pl.when(j == 0)
            def _():
                for h in range(KV):
                    kv[chip, 0, h] = turned(h)

            @pl.when(j == 1)
            def _():
                for h in range(KV):
                    kv[chip, 1, h] = sc[:, h * HEAD : (h + 1) * HEAD].astype(BF16)
                for b in range(1, CHIPS):
                    @pl.when(b > chip)
                    def _():
                        send(b).start()

            @pl.when(j >= 2)
            def _():
                for h in range(4):
                    q_all[(j - 2) * 4 + h] = turned(h)

            return 0

        lax.fori_loop(0, NQKV, block, 0)

    def send(b):
        return pltpu.make_async_remote_copy(src_ref=kv.at[chip], dst_ref=kv.at[chip], send_sem=kvs.at[b], recv_sem=kvr.at[chip],
                                            device_id={"sp": 2 * b + core}, device_id_type=MESH)

    def received(b):
        return pltpu.make_async_remote_copy(src_ref=kv.at[b], dst_ref=kv.at[b], send_sem=kvs.at[b], recv_sem=kvr.at[b],
                                            device_id={"sp": partner}, device_id_type=MESH)

    pl.run_scoped(project, pltpu.VMEM((TOK, D), BF16), pltpu.VMEM((TOK, W), F32))

    def attention(top_s, mix_s):
        ones = jnp.ones((8, TOK), BF16)

        def own(g, _):
            k, vt = kv[chip, 0, g], jnp.concatenate([kv[chip, 1, g].T, ones], 0)
            ok = lax.broadcasted_iota(jnp.int32, (OWN, OWN), 0) <= lax.broadcasted_iota(jnp.int32, (OWN, OWN), 1)
            pieces = [(h, part) for h in range(G) for part in range(2)]
            scores = [_dot(k[: (part + 1) * OWN], q_all[g * G + h, part * OWN : (part + 1) * OWN, :], 1, 1) for h, part in pieces]
            weights = []
            for (h, part), s in zip(pieces, scores):
                tri = jnp.where(ok, s[part * OWN :], HIDDEN)
                s = tri if part == 0 else jnp.concatenate([s[:OWN], tri], 0)
                top = s.max(axis=0, keepdims=True)
                top_s[g * G + h, :, part * OWN : (part + 1) * OWN] = top
                weights.append(jnp.exp2((s - top) * SCALE2).astype(BF16))
            for (h, part), p in zip(pieces, weights):
                mix_s[g * G + h, :, part * OWN : (part + 1) * OWN] = _dot(vt[:, : (part + 1) * OWN], p, 1, 0)
            return 0

        lax.fori_loop(0, KV, own, 0)

        def earlier(i, _):
            b = chip - i
            received(b).wait_recv()

            def heads(g, _):
                k, vt = kv[b, 0, g], jnp.concatenate([kv[b, 1, g].T, ones], 0)
                scores = [_dot(k, q_all[g * G + h], 1, 1) for h in range(G)]
                weights, keeps = [], []
                for h, s in enumerate(scores):
                    old = top_s[g * G + h]
                    top = jnp.maximum(old, s.max(axis=0, keepdims=True))
                    top_s[g * G + h] = top
                    weights.append(jnp.exp2((s - top) * SCALE2).astype(BF16))
                    keeps.append(jnp.exp2((old - top) * SCALE2))
                for h, (p, keep) in enumerate(zip(weights, keeps)):
                    mix_s[g * G + h] = mix_s[g * G + h] * keep + _dot(vt, p, 1, 0)
                return 0

            lax.fori_loop(0, KV, heads, 0)
            return 0

        lax.fori_loop(1, chip + 1, earlier, 0)

        def finish(g, _):
            for h in range(G):
                total = mix_s[g * G + h, HEAD : HEAD + 1, :]
                out = (mix_s[g * G + h, :HEAD, :] * (1 / total)).astype(BF16).T
                o_all[:, pl.ds(pl.multiple_of((g * G + h) * HEAD, HEAD), HEAD)] = out
            return 0

        lax.fori_loop(0, KV, finish, 0)

    pl.run_scoped(attention, pltpu.VMEM((NH, 1, TOK), F32), pltpu.VMEM((NH, HEAD + 8, TOK), F32))

    def output(yblk, ybuf):
        def cross(n):
            slot = lax.rem(n, 3)
            return pltpu.make_async_remote_copy(
                src_ref=yblk.at[slot, pl.ds(pl.multiple_of((1 - core) * OWN, OWN), OWN)], dst_ref=yrecv.at[n],
                send_sem=yss.at[slot], recv_sem=yrs.at[n], device_id={"sp": partner}, device_id_type=MESH)

        def store(n):
            slot = lax.rem(n, 2)
            return pltpu.make_async_copy(ybuf.at[slot], y_ref.at[:, pl.ds(pl.multiple_of(n * W, W), W)], osem.at[slot])

        def settle(n):
            cross(n).wait()

            @pl.when(n >= 2)
            def _():
                store(n - 2).wait()

            own = yblk[lax.rem(n, 3), pl.ds(pl.multiple_of(core * OWN, OWN), OWN), :]
            res = x_own[:, pl.ds(pl.multiple_of(n * W, W), W)].astype(F32)
            ybuf[lax.rem(n, 2)] = (res + (own + yrecv[n])).astype(BF16)
            store(n).start()

        def block(n, _):
            slot = lax.rem(n + 4, SLOTS)
            take(wo_ref, 0, 0, slot).wait()
            yblk[lax.rem(n, 3)] = _dot(o_all[...], wbuf[slot], 1, 0)
            cross(n).start()

            @pl.when(n + SLOTS < NOUT)
            def _():
                take_out(n + SLOTS, slot).start()

            @pl.when(n >= 1)
            def _():
                settle(n - 1)

            return 0

        lax.fori_loop(0, NOUT, block, 0)
        settle(NOUT - 1)
        store(NOUT - 2).wait()
        store(NOUT - 1).wait()

    pl.run_scoped(output, pltpu.VMEM((3, TOK, W), F32), pltpu.VMEM((2, OWN, W), BF16))

    x_swap.wait_send()
    for b in range(1, CHIPS):
        @pl.when(b > chip)
        def _():
            send(b).wait_send()


def solution(mesh):
    def step(x, gain, wq, wk, wv, wo):
        half = HEAD // 2
        freq = THETA ** (-jnp.arange(half, dtype=F32) / half)
        freq = jnp.concatenate([freq, freq])[None]
        any_, vmem = pl.BlockSpec(memory_space=pl.ANY), pl.BlockSpec(memory_space=pltpu.VMEM)
        dma = pltpu.SemaphoreType.DMA
        return pl.pallas_call(
            _kernel,
            out_shape=jax.ShapeDtypeStruct((OWN, D), BF16),
            in_specs=[any_, vmem, vmem, any_, any_, any_, any_],
            out_specs=any_,
            scratch_shapes=[
                pltpu.VMEM((OWN, D), BF16), pltpu.VMEM((OWN, D), BF16), pltpu.VMEM((SLOTS, HALF, W), BF16),
                pltpu.VMEM((CHIPS, 2, KV, TOK, HEAD), BF16), pltpu.VMEM((NH, TOK, HEAD), BF16), pltpu.VMEM((TOK, HALF), BF16),
                pltpu.VMEM((NOUT, OWN, W), F32), pltpu.VMEM((TOK, HEAD), F32), pltpu.VMEM((TOK, HEAD), F32),
                dma, dma, dma, dma((SLOTS,)), dma((CHIPS,)), dma((CHIPS,)), dma((3,)), dma((NOUT,)), dma((2,)),
            ],
            compiler_params=pltpu.CompilerParams(collective_id=0, has_side_effects=True, vmem_limit_bytes=67043328),
        )(x, gain[None], freq, wq, wk, wv, wo)

    tokens, whole = P(("dp", "sp"), None), P(None, None)
    return jax.shard_map(
        step,
        mesh=mesh,
        in_specs=(tokens, P(None), whole, whole, whole, whole),
        out_specs=tokens,
        check_vma=False,
    )
```

```python
import math

import jax
import jax.numpy as jnp
from jax import lax
from jax.experimental import pallas as pl
from jax.experimental.pallas import tpu as pltpu
from jax.sharding import PartitionSpec as P

HEAD = 128
THETA = 10000
LOG2E = 1.4426950408889634
HIDDEN = -1e30
MESH = pl.DeviceIdType.MESH
F32, BF16 = jnp.float32, jnp.bfloat16

D = 6144
OWN = 256
TOK = 512
CHIPS = 4
KV = 4
G = 6
NH = KV * G
HALF = D // 2
W = 512
SLOTS = 6
NQ = HALF // W
NOUT = D // W
ROWS = 64
NCH = OWN // ROWS
LAG = 2
SCALE2 = HEAD**-0.5 * LOG2E


def _dot(a, b, ca, cb):
    return lax.dot_general(a, b, (((ca,), (cb,)), ((), ())), preferred_element_type=F32)


def _kernel(x_ref, gain_ref, wq_ref, wk_ref, wv_ref, wo_ref, y_ref,
            x_own, a_all, wbuf, kv, q_all, yrecv, cos_s, sin_s, gain_s,
            xsem, as_sem, ar_sem, wsem, kvs, kvr, yss, yrs, osem):
    me = lax.axis_index("sp")
    chip, core = me // 2, me % 2
    partner = me + 1 - 2 * core
    o_all = a_all.at[:, :HALF]

    barrier = pltpu.get_barrier_semaphore()
    for d in range(1, 8):
        pl.semaphore_signal(barrier, inc=1, device_id={"sp": (me + d) % 8}, device_id_type=MESH)

    def take(w_ref, row, col, slot):
        return pltpu.make_async_copy(w_ref.at[pl.ds(row, HALF), pl.ds(col, W)], wbuf.at[slot], wsem.at[slot])

    def take_full(w_ref, col, pair):
        col = pl.multiple_of(col, W)
        take(w_ref, 0, col, 2 * pair).start()
        take(w_ref, HALF, col, 2 * pair + 1).start()

    def arrived(pair):
        for i in range(2):
            take(wq_ref, 0, 0, 2 * pair + i).wait()

    def take_out(n, slot):
        return take(wo_ref, pl.multiple_of(core * HALF, HALF), pl.multiple_of(n * W, W), slot)

    def own_rows(i):
        return pl.ds(pl.multiple_of(i * ROWS, ROWS), ROWS)

    def chip_rows(part, i):
        return pl.ds(pl.multiple_of(part * OWN + i * ROWS, ROWS), ROWS)

    def part_rows(part):
        return pl.ds(pl.multiple_of(part * OWN, OWN), OWN)

    def x_in(i):
        return pltpu.make_async_copy(x_ref.at[own_rows(i)], x_own.at[own_rows(i)], xsem.at[i])

    def swap(part, i):
        rows = chip_rows(part, i)
        return pltpu.make_async_remote_copy(src_ref=a_all.at[rows], dst_ref=a_all.at[rows], send_sem=as_sem.at[i], recv_sem=ar_sem.at[i],
                                            device_id={"sp": partner}, device_id_type=MESH)

    def send(src, target, k):
        return pltpu.make_async_remote_copy(src_ref=kv.at[src], dst_ref=kv.at[src], send_sem=kvs.at[k], recv_sem=kvr.at[src],
                                            device_id={"sp": 2 * target + core}, device_id_type=MESH)

    def received(src):
        send(src, 0, 0).wait_recv()

    for i in range(NCH):
        x_in(i).start()
    take_full(wk_ref, core * W, 0)
    take_full(wv_ref, core * W, 1)
    take_full(wq_ref, core * HALF, 2)

    gain_s[...] = jnp.concatenate([gain_ref[i : i + 1, :].astype(F32) for i in range(D // HEAD)], 1)
    lane = lax.broadcasted_iota(jnp.int32, (TOK, HEAD), 1)
    place = (chip * TOK + lax.broadcasted_iota(jnp.int32, (TOK, HEAD), 0)).astype(F32)
    angle = place * jnp.exp(lax.rem(lane, HEAD // 2).astype(F32) * (-math.log(THETA) * 2 / HEAD))
    cos_s[...] = jnp.cos(angle)
    sin_s[...] = jnp.where(lane < HEAD // 2, -1.0, 1.0) * jnp.sin(angle)

    pl.semaphore_wait(barrier, 7)

    def norm(i, _):
        x_in(i).wait()
        total = jnp.zeros((ROWS, HEAD), F32)
        for c in range(D // HEAD):
            wide = x_own[own_rows(i), c * HEAD : (c + 1) * HEAD].astype(F32)
            total += wide * wide
        scale = lax.rsqrt(jnp.sum(total, -1, keepdims=True) * (1 / D) + 1e-6)
        for c in range(D // HEAD):
            at = slice(c * HEAD, (c + 1) * HEAD)
            a_all[chip_rows(core, i), at] = (x_own[own_rows(i), at].astype(F32) * scale * gain_s[:, at]).astype(BF16)
        swap(core, i).start()
        return 0

    lax.fori_loop(0, NCH, norm, 0)

    def times(a, b, pair):
        return _dot(a, wbuf[2 * pair], 1, 0) + _dot(b, wbuf[2 * pair + 1], 1, 0)

    def turned(t, rows):
        t = t.astype(BF16).astype(F32)
        return (t * cos_s[rows, :] + pltpu.roll(t, HEAD // 2, 1) * sin_s[rows, :]).astype(BF16)

    def project(sc_a, sc_b):
        scs = [sc_a, sc_b]
        arrived(0)
        arrived(1)

        def keys(p, _):
            part = jnp.where(p == 0, core, 1 - core)

            @pl.when(p == 1)
            def _():
                for i in range(NCH):
                    swap(1 - core, i).wait_recv()

            rows = part_rows(part)
            src = 2 * chip + part
            sc_a[:OWN] = times(a_all[rows, :HALF], a_all[rows, HALF:], 0)
            sc_a[OWN:] = times(a_all[rows, :HALF], a_all[rows, HALF:], 1)
            for h in range(KV):
                at = slice(h * HEAD, (h + 1) * HEAD)
                kv[src, 0, h] = turned(sc_a[:OWN, at], rows)
                kv[src, 1, h] = sc_a[OWN:, at].astype(BF16)

            @pl.when(chip == 0)
            def _():
                send(src, 1, p).start()
                send(src, 2, 2 + p).start()

            @pl.when((chip == 1) | (chip == 2))
            def _():
                send(src, 3, p).start()

            return 0

        lax.fori_loop(0, 2, keys, 0)
        take_full(wq_ref, core * HALF + W, 0)
        take_full(wq_ref, core * HALF + 2 * W, 1)

        def epilogue(j):
            for h in range(4):
                q_all[j * 4 + h] = turned(scs[j % 2][:, h * HEAD : (h + 1) * HEAD], slice(None))

        for j in range(NQ):
            pair = (j + 2) % 3
            arrived(pair)
            if j:
                epilogue(j - 1)
            scs[j % 2][...] = times(a_all[:, :HALF], a_all[:, HALF:], pair)
            if j + 3 < NQ:
                take_full(wq_ref, core * HALF + (j + 3) * W, pair)
            else:
                for i in range(2):
                    take_out(2 * (j + 3 - NQ) + i, 2 * pair + i).start()
            if j == NQ - 2:
                relay(0)
        epilogue(NQ - 1)

    def relay(k):
        @pl.when(chip == 3)
        def _():
            src = 2 + jnp.where(core == k, 0, 1)
            received(src)
            send(src, 2, k).start()

        if k:
            @pl.when((chip == 1) | (chip == 2))
            def _():
                src = chip - 1
                received(src)
                send(src, 3, 2).start()

    pl.run_scoped(project, pltpu.VMEM((TOK, W), F32), pltpu.VMEM((TOK, W), F32))
    relay(1)

    def attention(top_s, mix_s):
        ones = jnp.ones((8, TOK), BF16)

        def pair_of(b, g):
            k = jnp.concatenate([kv[2 * b, 0, g], kv[2 * b + 1, 0, g]], 0)
            v = jnp.concatenate([kv[2 * b, 1, g], kv[2 * b + 1, 1, g]], 0)
            return k, jnp.concatenate([v.T, ones], 0)

        def own(g, _):
            k, vt = pair_of(chip, g)
            ok = lax.broadcasted_iota(jnp.int32, (OWN, OWN), 0) <= lax.broadcasted_iota(jnp.int32, (OWN, OWN), 1)
            pieces = [(h, part) for h in range(G) for part in range(2)]
            scores = [_dot(k[: (part + 1) * OWN], q_all[g * G + h, part * OWN : (part + 1) * OWN, :], 1, 1) for h, part in pieces]
            weights = []
            for (h, part), s in zip(pieces, scores):
                tri = jnp.where(ok, s[part * OWN :], HIDDEN)
                s = tri if part == 0 else jnp.concatenate([s[:OWN], tri], 0)
                top = s.max(axis=0, keepdims=True)
                top_s[g * G + h, :, part * OWN : (part + 1) * OWN] = top
                weights.append(jnp.exp2((s - top) * SCALE2).astype(BF16))
            for (h, part), p in zip(pieces, weights):
                mix_s[g * G + h, :, part * OWN : (part + 1) * OWN] = _dot(vt[:, : (part + 1) * OWN], p, 1, 0)
            return 0

        lax.fori_loop(0, KV, own, 0)

        def earlier(i, _):
            b = jnp.where(chip == 2, (i - 1), chip - i)

            @pl.when(jnp.logical_not(((chip == 3) & (b == 1)) | ((chip == 1) & (b == 0))))
            def _():
                @pl.when(jnp.logical_not((chip == 2) & (b == 0)))
                def _():
                    received(2 * b + 1)
                received(2 * b)

            @pl.when((chip == 1) & (b == 0))
            def _():
                received(2 * b + 1)

            def heads(g, _):
                k, vt = pair_of(b, g)
                scores = [_dot(k, q_all[g * G + h], 1, 1) for h in range(G)]
                weights, keeps = [], []
                for h, s in enumerate(scores):
                    old = top_s[g * G + h]
                    top = jnp.maximum(old, s.max(axis=0, keepdims=True))
                    top_s[g * G + h] = top
                    weights.append(jnp.exp2((s - top) * SCALE2).astype(BF16))
                    keeps.append(jnp.exp2((old - top) * SCALE2))
                for h, (p, keep) in enumerate(zip(weights, keeps)):
                    mix_s[g * G + h] = mix_s[g * G + h] * keep + _dot(vt, p, 1, 0)
                return 0

            lax.fori_loop(0, KV, heads, 0)
            return 0

        lax.fori_loop(1, chip + 1, earlier, 0)

        def finish(g, _):
            for h in range(G):
                total = mix_s[g * G + h, HEAD : HEAD + 1, :]
                out = (mix_s[g * G + h, :HEAD, :] * (1 / total)).astype(BF16).T
                o_all[:, pl.ds(pl.multiple_of((g * G + h) * HEAD, HEAD), HEAD)] = out
            return 0

        lax.fori_loop(0, KV, finish, 0)

    for i in range(NCH):
        swap(core, i).wait_send()
    pl.run_scoped(attention, pltpu.VMEM((NH, 1, TOK), F32), pltpu.VMEM((NH, HEAD + 8, TOK), F32))

    def output(yblk, ybuf):
        ring = LAG + 2

        def cross(n):
            slot = lax.rem(n, ring)
            return pltpu.make_async_remote_copy(src_ref=yblk.at[slot, part_rows(1 - core)], dst_ref=yrecv.at[n], send_sem=yss.at[slot],
                                                recv_sem=yrs.at[n], device_id={"sp": partner}, device_id_type=MESH)

        def store(n):
            slot = lax.rem(n, 2)
            return pltpu.make_async_copy(ybuf.at[slot], y_ref.at[:, pl.ds(pl.multiple_of(n * W, W), W)], osem.at[slot])

        def settle(n):
            own = yblk[lax.rem(n, ring), part_rows(core), :]
            res = x_own[:, pl.ds(pl.multiple_of(n * W, W), W)].astype(F32)
            ybuf[lax.rem(n, 2)] = (res + (own + yrecv[n])).astype(BF16)

        def ready(n):
            cross(n).wait()

            @pl.when(n >= 2)
            def _():
                store(n - 2).wait()

        def block(n, settles):
            slot = lax.rem(n + 4, SLOTS)
            take(wo_ref, 0, 0, slot).wait()
            if settles:
                ready(n - LAG)
                settle(n - LAG)
            yblk[lax.rem(n, ring)] = _dot(o_all[...], wbuf[slot], 1, 0)
            cross(n).start()
            if settles:
                store(n - LAG).start()

            @pl.when(n + SLOTS < NOUT)
            def _():
                take_out(n + SLOTS, slot).start()

        for n in range(LAG):
            block(jnp.int32(n), False)
        lax.fori_loop(LAG, NOUT, lambda n, _: (block(n, True), 0)[1], 0)
        for n in range(NOUT - LAG, NOUT):
            ready(jnp.int32(n))
            settle(jnp.int32(n))
            store(jnp.int32(n)).start()
        for n in range(NOUT - 2, NOUT):
            store(jnp.int32(n)).wait()

    pl.run_scoped(output, pltpu.VMEM((LAG + 2, TOK, W), F32), pltpu.VMEM((2, OWN, W), BF16))

    @pl.when(chip == 0)
    def _():
        for k in range(4):
            send(0, 0, k).wait_send()

    @pl.when((chip == 1) | (chip == 2))
    def _():
        for k in range(3):
            send(0, 0, k).wait_send()

    @pl.when(chip == 3)
    def _():
        for k in range(2):
            send(0, 0, k).wait_send()


def solution(mesh):
    def step(x, gain, wq, wk, wv, wo):
        any_, vmem = pl.BlockSpec(memory_space=pl.ANY), pl.BlockSpec(memory_space=pltpu.VMEM)
        dma = pltpu.SemaphoreType.DMA
        return pl.pallas_call(
            _kernel,
            out_shape=jax.ShapeDtypeStruct((OWN, D), BF16),
            in_specs=[any_, vmem, any_, any_, any_, any_],
            out_specs=any_,
            scratch_shapes=[
                pltpu.VMEM((OWN, D), BF16), pltpu.VMEM((TOK, D), BF16), pltpu.VMEM((SLOTS, HALF, W), BF16),
                pltpu.VMEM((2 * CHIPS, 2, KV, OWN, HEAD), BF16), pltpu.VMEM((NH, TOK, HEAD), BF16),
                pltpu.VMEM((NOUT, OWN, W), F32), pltpu.VMEM((TOK, HEAD), F32), pltpu.VMEM((TOK, HEAD), F32), pltpu.VMEM((1, D), F32),
                dma((NCH,)), dma((NCH,)), dma((NCH,)), dma((SLOTS,)), dma((4,)), dma((2 * CHIPS,)), dma((LAG + 2,)), dma((NOUT,)), dma((2,)),
            ],
            compiler_params=pltpu.CompilerParams(collective_id=0, has_side_effects=True, vmem_limit_bytes=67043328),
        )(x, gain.reshape(D // HEAD, HEAD), wq, wk, wv, wo)

    tokens, whole = P(("dp", "sp"), None), P(None, None)
    return jax.shard_map(
        step,
        mesh=mesh,
        in_specs=(tokens, P(None), whole, whole, whole, whole),
        out_specs=tokens,
        check_vma=False,
    )
```

```python
import math

import jax
import jax.numpy as jnp
from jax import lax
from jax.experimental import pallas as pl
from jax.experimental.pallas import tpu as pltpu
from jax.sharding import PartitionSpec as P

HEAD = 128
THETA = 10000
LOG2E = 1.4426950408889634
HIDDEN = -1e30
MESH = pl.DeviceIdType.MESH
F32, BF16 = jnp.float32, jnp.bfloat16

D = 6144
OWN = 256
TOK = 512
CHIPS = 4
KV = 4
G = 6
NH = KV * G
HALF = D // 2
W = 512
SLOTS = 6
NQ = HALF // W
NOUT = D // W
ROWS = 64
NCH = OWN // ROWS
STRIP = 256
AHEAD = 3
LAG = 2
SCALE2 = HEAD**-0.5 * LOG2E


def _dot(a, b, ca, cb):
    return lax.dot_general(a, b, (((ca,), (cb,)), ((), ())), preferred_element_type=F32)


def _kernel(x_ref, gain_ref, wq_ref, wk_ref, wv_ref, wo_ref, y_ref,
            x_own, a_all, wbuf, kv, q_all, yrecv, cos_s, sin_s, gain_s,
            xsem, as_sem, ar_sem, wsem, kvs, kvr, yss, yrs, osem):
    me = lax.axis_index("sp")
    chip, core = me // 2, me % 2
    partner = me + 1 - 2 * core
    o_all = a_all.at[:, :HALF]

    barrier = pltpu.get_barrier_semaphore()
    for d in range(1, 8):
        pl.semaphore_signal(barrier, inc=1, device_id={"sp": (me + d) % 8}, device_id_type=MESH)

    def take(w_ref, row, col, slot):
        return pltpu.make_async_copy(w_ref.at[pl.ds(row, HALF), pl.ds(col, W)], wbuf.at[slot], wsem.at[slot])

    def take_queries(j):
        col = pl.multiple_of(core * HALF + j * W, W)
        for i in range(2):
            take(wq_ref, i * HALF, col, 2 * (j % 3) + i).start()

    def arrived(pair):
        for i in range(2):
            take(wq_ref, 0, 0, 2 * pair + i).wait()

    def take_out(n, slot):
        return take(wo_ref, pl.multiple_of(core * HALF, HALF), pl.multiple_of(n * W, W), slot)

    def own_rows(i):
        return pl.ds(pl.multiple_of(i * ROWS, ROWS), ROWS)

    def chip_rows(part, i):
        return pl.ds(pl.multiple_of(part * OWN + i * ROWS, ROWS), ROWS)

    def part_rows(part):
        return pl.ds(pl.multiple_of(part * OWN, OWN), OWN)

    def x_in(i):
        return pltpu.make_async_copy(x_ref.at[own_rows(i)], x_own.at[own_rows(i)], xsem.at[i])

    def swap(part, i):
        rows = chip_rows(part, i)
        return pltpu.make_async_remote_copy(src_ref=a_all.at[rows], dst_ref=a_all.at[rows], send_sem=as_sem.at[i], recv_sem=ar_sem.at[i],
                                            device_id={"sp": partner}, device_id_type=MESH)

    def send(src, target, k):
        return pltpu.make_async_remote_copy(src_ref=kv.at[src], dst_ref=kv.at[src], send_sem=kvs.at[k], recv_sem=kvr.at[src],
                                            device_id={"sp": 2 * target + core}, device_id_type=MESH)

    def received(src):
        send(src, 0, 0).wait_recv()

    def prepare():
        gain_s[...] = jnp.concatenate([gain_ref[i : i + 1, :].astype(F32) for i in range(D // HEAD)], 1)
        lane = lax.broadcasted_iota(jnp.int32, (TOK, HEAD), 1)
        place = (chip * TOK + lax.broadcasted_iota(jnp.int32, (TOK, HEAD), 0)).astype(F32)
        angle = place * jnp.exp(lax.rem(lane, HEAD // 2).astype(F32) * (-math.log(THETA) * 2 / HEAD))
        cos_s[...] = jnp.cos(angle)
        sin_s[...] = jnp.where(lane < HEAD // 2, -1.0, 1.0) * jnp.sin(angle)

    def norm(i, _):
        x_in(i).wait()
        total = jnp.zeros((ROWS, HEAD), F32)
        for c in range(D // HEAD):
            wide = x_own[own_rows(i), c * HEAD : (c + 1) * HEAD].astype(F32)
            total += wide * wide
        scale = lax.rsqrt(jnp.sum(total, -1, keepdims=True) * (1 / D) + 1e-6)
        for c in range(D // HEAD):
            at = slice(c * HEAD, (c + 1) * HEAD)
            a_all[chip_rows(core, i), at] = (x_own[own_rows(i), at].astype(F32) * scale * gain_s[:, at]).astype(BF16)
        swap(core, i).start()
        return 0

    def times(rows, low, high):
        return _dot(a_all[rows, :HALF], low[...], 1, 0) + _dot(a_all[rows, HALF:], high[...], 1, 0)

    def turned(t, rows):
        t = t.astype(BF16).astype(F32)
        return (t * cos_s[rows, :] + pltpu.roll(t, HEAD // 2, 1) * sin_s[rows, :]).astype(BF16)

    def project(sc_a, sc_b, wkv, wkv_sem):
        scs = [sc_a, sc_b]

        def take_kv(w_ref, i):
            return pltpu.make_async_copy(w_ref.at[pl.ds(i % 2 * HALF, HALF), pl.ds(pl.multiple_of(core * W, W), W)], wkv.at[i], wkv_sem.at[i])

        for i in range(NCH):
            x_in(i).start()
        for i in range(4):
            take_kv([wk_ref, wv_ref][i // 2], i).start()
        prepare()
        pl.semaphore_wait(barrier, 7)
        lax.fori_loop(0, NCH, norm, 0)
        take_queries(0)
        for i in range(4):
            take_kv(wk_ref, i).wait()

        def keys(p, _):
            part = jnp.where(p == 0, core, 1 - core)

            @pl.when(p == 1)
            def _():
                take_queries(1)
                take_queries(2)
                for i in range(NCH):
                    swap(1 - core, i).wait_recv()

            rows = part_rows(part)
            src = 2 * chip + part
            sc_a[:OWN] = times(rows, wkv.at[0], wkv.at[1])
            sc_a[OWN:] = times(rows, wkv.at[2], wkv.at[3])
            for h in range(KV):
                at = slice(h * HEAD, (h + 1) * HEAD)
                kv[src, 0, h] = turned(sc_a[:OWN, at], rows)
                kv[src, 1, h] = sc_a[OWN:, at].astype(BF16)

            @pl.when(chip == 0)
            def _():
                send(src, 1, p).start()
                send(src, 2, 2 + p).start()

            @pl.when((chip == 1) | (chip == 2))
            def _():
                send(src, 3, p).start()

            return 0

        lax.fori_loop(0, 2, keys, 0)

        def epilogue(j):
            for h in range(4):
                q_all[j * 4 + h] = turned(scs[j % 2][:, h * HEAD : (h + 1) * HEAD], slice(None))

        for j in range(NQ):
            pair = j % 3
            arrived(pair)
            if j:
                epilogue(j - 1)
            scs[j % 2][...] = times(slice(None), wbuf.at[2 * pair], wbuf.at[2 * pair + 1])
            if j + 3 < NQ:
                take_queries(j + 3)
            else:
                for i in range(2):
                    take_out(2 * (j + 3 - NQ) + i, 2 * pair + i).start()
            if j == 2:
                relay(0)
        epilogue(NQ - 1)

    def relay(k):
        @pl.when(chip == 3)
        def _():
            src = 2 + jnp.where(core == k, 0, 1)
            received(src)
            send(src, 2, k).start()

        if k:
            @pl.when((chip == 1) | (chip == 2))
            def _():
                src = chip - 1
                received(src)
                send(src, 3, 2).start()

    pl.run_scoped(project, pltpu.VMEM((TOK, W), F32), pltpu.VMEM((TOK, W), F32), pltpu.VMEM((4, HALF, W), BF16), pltpu.SemaphoreType.DMA((4,)))
    relay(1)

    def attention(top_s, mix_s):
        ones = jnp.ones((8, TOK), BF16)

        def pair_of(b, g):
            k = jnp.concatenate([kv[2 * b, 0, g], kv[2 * b + 1, 0, g]], 0)
            v = jnp.concatenate([kv[2 * b, 1, g], kv[2 * b + 1, 1, g]], 0)
            return k, jnp.concatenate([v.T, ones], 0)

        def own(g, _):
            k, vt = pair_of(chip, g)
            ok = lax.broadcasted_iota(jnp.int32, (OWN, OWN), 0) <= lax.broadcasted_iota(jnp.int32, (OWN, OWN), 1)
            pieces = [(h, part) for h in range(G) for part in range(2)]
            scores = [_dot(k[: (part + 1) * OWN], q_all[g * G + h, part * OWN : (part + 1) * OWN, :], 1, 1) for h, part in pieces]
            weights = []
            for (h, part), s in zip(pieces, scores):
                tri = jnp.where(ok, s[part * OWN :], HIDDEN)
                s = tri if part == 0 else jnp.concatenate([s[:OWN], tri], 0)
                top = s.max(axis=0, keepdims=True)
                top_s[g * G + h, :, part * OWN : (part + 1) * OWN] = top
                weights.append(jnp.exp2((s - top) * SCALE2).astype(BF16))
            for (h, part), p in zip(pieces, weights):
                mix_s[g * G + h, :, part * OWN : (part + 1) * OWN] = _dot(vt[:, : (part + 1) * OWN], p, 1, 0)
            return 0

        lax.fori_loop(0, KV, own, 0)

        def earlier(i, _):
            b = jnp.where(chip == 2, (i - 1), chip - i)

            @pl.when(jnp.logical_not(((chip == 3) & (b == 1)) | ((chip == 1) & (b == 0))))
            def _():
                @pl.when(jnp.logical_not((chip == 2) & (b == 0)))
                def _():
                    received(2 * b + 1)
                received(2 * b)

            @pl.when((chip == 1) & (b == 0))
            def _():
                received(2 * b + 1)

            pieces = [(g, g * G + h, slice(at, at + STRIP)) for g in range(KV) for h in range(G) for at in range(0, TOK, STRIP)]
            pairs = [pair_of(b, g) for g in range(KV)]
            scores, weights = {}, {}
            for i in range(len(pieces) + 2 * AHEAD):
                if i < len(pieces):
                    g, h, at = pieces[i]
                    scores[i] = _dot(pairs[g][0], q_all[h, at, :], 1, 1)
                if 0 <= i - AHEAD < len(pieces):
                    g, h, at = pieces[i - AHEAD]
                    s, old = scores.pop(i - AHEAD), top_s[h, :, at]
                    top = jnp.maximum(old, s.max(axis=0, keepdims=True))
                    top_s[h, :, at] = top
                    weights[i - AHEAD] = jnp.exp2((s - top) * SCALE2).astype(BF16), jnp.exp2((old - top) * SCALE2)
                if 0 <= i - 2 * AHEAD < len(pieces):
                    g, h, at = pieces[i - 2 * AHEAD]
                    p, keep = weights.pop(i - 2 * AHEAD)
                    mix_s[h, :, at] = mix_s[h, :, at] * keep + _dot(pairs[g][1], p, 1, 0)

            return 0

        lax.fori_loop(1, chip + 1, earlier, 0)

        def finish(g, _):
            for h in range(G):
                total = mix_s[g * G + h, HEAD : HEAD + 1, :]
                out = (mix_s[g * G + h, :HEAD, :] * (1 / total)).astype(BF16).T
                o_all[:, pl.ds(pl.multiple_of((g * G + h) * HEAD, HEAD), HEAD)] = out
            return 0

        lax.fori_loop(0, KV, finish, 0)

    for i in range(NCH):
        swap(core, i).wait_send()
    pl.run_scoped(attention, pltpu.VMEM((NH, 1, TOK), F32), pltpu.VMEM((NH, HEAD + 8, TOK), F32))

    def output(yblk, ybuf):
        ring = LAG + 2

        def cross(n):
            slot = lax.rem(n, ring)
            return pltpu.make_async_remote_copy(src_ref=yblk.at[slot, part_rows(1 - core)], dst_ref=yrecv.at[n], send_sem=yss.at[slot],
                                                recv_sem=yrs.at[n], device_id={"sp": partner}, device_id_type=MESH)

        def store(n):
            slot = lax.rem(n, 2)
            return pltpu.make_async_copy(ybuf.at[slot], y_ref.at[:, pl.ds(pl.multiple_of(n * W, W), W)], osem.at[slot])

        def settle(n):
            own = yblk[lax.rem(n, ring), part_rows(core), :]
            res = x_own[:, pl.ds(pl.multiple_of(n * W, W), W)].astype(F32)
            ybuf[lax.rem(n, 2)] = (res + (own + yrecv[n])).astype(BF16)

        def ready(n):
            cross(n).wait()

            @pl.when(n >= 2)
            def _():
                store(n - 2).wait()

        def block(n, settles):
            slot = lax.rem(n, SLOTS)
            take(wo_ref, 0, 0, slot).wait()
            if settles:
                ready(n - LAG)
                settle(n - LAG)
            yblk[lax.rem(n, ring)] = _dot(o_all[...], wbuf[slot], 1, 0)
            cross(n).start()
            if settles:
                store(n - LAG).start()

            @pl.when(n + SLOTS < NOUT)
            def _():
                take_out(n + SLOTS, slot).start()

        for n in range(LAG):
            block(jnp.int32(n), False)
        lax.fori_loop(LAG, NOUT, lambda n, _: (block(n, True), 0)[1], 0)
        for n in range(NOUT - LAG, NOUT):
            ready(jnp.int32(n))
            settle(jnp.int32(n))
            store(jnp.int32(n)).start()
        for n in range(NOUT - 2, NOUT):
            store(jnp.int32(n)).wait()

    pl.run_scoped(output, pltpu.VMEM((LAG + 2, TOK, W), F32), pltpu.VMEM((2, OWN, W), BF16))

    @pl.when(chip == 0)
    def _():
        for k in range(4):
            send(0, 0, k).wait_send()

    @pl.when((chip == 1) | (chip == 2))
    def _():
        for k in range(3):
            send(0, 0, k).wait_send()

    @pl.when(chip == 3)
    def _():
        for k in range(2):
            send(0, 0, k).wait_send()


def solution(mesh):
    def step(x, gain, wq, wk, wv, wo):
        any_, vmem = pl.BlockSpec(memory_space=pl.ANY), pl.BlockSpec(memory_space=pltpu.VMEM)
        dma = pltpu.SemaphoreType.DMA
        return pl.pallas_call(
            _kernel,
            out_shape=jax.ShapeDtypeStruct((OWN, D), BF16),
            in_specs=[any_, vmem, any_, any_, any_, any_],
            out_specs=any_,
            scratch_shapes=[
                pltpu.VMEM((OWN, D), BF16), pltpu.VMEM((TOK, D), BF16), pltpu.VMEM((SLOTS, HALF, W), BF16),
                pltpu.VMEM((2 * CHIPS, 2, KV, OWN, HEAD), BF16), pltpu.VMEM((NH, TOK, HEAD), BF16),
                pltpu.VMEM((NOUT, OWN, W), F32), pltpu.VMEM((TOK, HEAD), F32), pltpu.VMEM((TOK, HEAD), F32), pltpu.VMEM((1, D), F32),
                dma((NCH,)), dma((NCH,)), dma((NCH,)), dma((SLOTS,)), dma((4,)), dma((2 * CHIPS,)), dma((LAG + 2,)), dma((NOUT,)), dma((2,)),
            ],
            compiler_params=pltpu.CompilerParams(collective_id=0, has_side_effects=True, vmem_limit_bytes=67043328),
        )(x, gain.reshape(D // HEAD, HEAD), wq, wk, wv, wo)

    tokens, whole = P(("dp", "sp"), None), P(None, None)
    return jax.shard_map(
        step,
        mesh=mesh,
        in_specs=(tokens, P(None), whole, whole, whole, whole),
        out_specs=tokens,
        check_vma=False,
    )
```

```python
import math

import jax
import jax.numpy as jnp
from jax import lax
from jax.experimental import pallas as pl
from jax.experimental.pallas import tpu as pltpu
from jax.sharding import PartitionSpec as P

HEAD = 128
THETA = 10000
LOG2E = 1.4426950408889634
HIDDEN = -1e30
MESH = pl.DeviceIdType.MESH
F32, BF16 = jnp.float32, jnp.bfloat16

D = 6144
OWN = 256
TOK = 512
CHIPS = 4
KV = 4
G = 6
NH = KV * G
HALF = D // 2
W = 512
SLOTS = 6
NQ = HALF // W
NOUT = D // W
ROWS = 64
NCH = OWN // ROWS
STRIP = 256
AHEAD = 3
LAG = 2
SCALE2 = HEAD**-0.5 * LOG2E


def _dot(a, b, ca, cb):
    return lax.dot_general(a, b, (((ca,), (cb,)), ((), ())), preferred_element_type=F32)


def _kernel(x_ref, gain_ref, wq_ref, wk_ref, wv_ref, wo_ref, y_ref,
            x_own, a_all, wbuf, kv, q_all, yrecv, cos_s, sin_s, gain_s,
            xsem, as_sem, ar_sem, wsem, kvs, kvr, yss, yrs, osem):
    me = lax.axis_index("sp")
    chip, core = me // 2, me % 2
    partner = me + 1 - 2 * core
    o_all = a_all.at[:, :HALF]

    barrier = pltpu.get_barrier_semaphore()
    for d in range(1, 8):
        pl.semaphore_signal(barrier, inc=1, device_id={"sp": (me + d) % 8}, device_id_type=MESH)

    def take(w_ref, row, col, slot):
        return pltpu.make_async_copy(w_ref.at[pl.ds(row, HALF), pl.ds(col, W)], wbuf.at[slot], wsem.at[slot])

    def take_queries(j):
        col = pl.multiple_of(core * HALF + j * W, W)
        for i in range(2):
            take(wq_ref, i * HALF, col, 2 * (j % 3) + i).start()

    def arrived(pair):
        for i in range(2):
            take(wq_ref, 0, 0, 2 * pair + i).wait()

    def take_out(n, slot):
        return take(wo_ref, pl.multiple_of(core * HALF, HALF), pl.multiple_of(n * W, W), slot)

    def own_rows(i):
        return pl.ds(pl.multiple_of(i * ROWS, ROWS), ROWS)

    def chip_rows(part, i):
        return pl.ds(pl.multiple_of(part * OWN + i * ROWS, ROWS), ROWS)

    def part_rows(part):
        return pl.ds(pl.multiple_of(part * OWN, OWN), OWN)

    def x_in(i):
        return pltpu.make_async_copy(x_ref.at[own_rows(i)], x_own.at[own_rows(i)], xsem.at[i])

    def swap(part, i):
        rows = chip_rows(part, i)
        return pltpu.make_async_remote_copy(src_ref=a_all.at[rows], dst_ref=a_all.at[rows], send_sem=as_sem.at[i], recv_sem=ar_sem.at[i],
                                            device_id={"sp": partner}, device_id_type=MESH)

    def send(src, target, k):
        return pltpu.make_async_remote_copy(src_ref=kv.at[src], dst_ref=kv.at[src], send_sem=kvs.at[k], recv_sem=kvr.at[src],
                                            device_id={"sp": 2 * target + core}, device_id_type=MESH)

    def received(src):
        send(src, 0, 0).wait_recv()

    def prepare():
        gain_s[...] = jnp.concatenate([gain_ref[i : i + 1, :].astype(F32) for i in range(D // HEAD)], 1)
        lane = lax.broadcasted_iota(jnp.int32, (TOK, HEAD), 1)
        place = (chip * TOK + lax.broadcasted_iota(jnp.int32, (TOK, HEAD), 0)).astype(F32)
        angle = place * jnp.exp(lax.rem(lane, HEAD // 2).astype(F32) * (-math.log(THETA) * 2 / HEAD))
        cos_s[...] = jnp.cos(angle)
        sin_s[...] = jnp.where(lane < HEAD // 2, -1.0, 1.0) * jnp.sin(angle)

    def norm(i, _):
        x_in(i).wait()
        total = jnp.zeros((ROWS, HEAD), F32)
        for c in range(D // HEAD):
            wide = x_own[own_rows(i), c * HEAD : (c + 1) * HEAD].astype(F32)
            total += wide * wide
        scale = lax.rsqrt(jnp.sum(total, -1, keepdims=True) * (1 / D) + 1e-6)
        for c in range(D // HEAD):
            at = slice(c * HEAD, (c + 1) * HEAD)
            a_all[chip_rows(core, i), at] = (x_own[own_rows(i), at].astype(F32) * scale * gain_s[:, at]).astype(BF16)
        swap(core, i).start()
        return 0

    def times(rows, low, high):
        return _dot(a_all[rows, :HALF], low[...], 1, 0) + _dot(a_all[rows, HALF:], high[...], 1, 0)

    def turned(t, rows):
        t = t.astype(BF16).astype(F32)
        return (t * cos_s[rows, :] + pltpu.roll(t, HEAD // 2, 1) * sin_s[rows, :]).astype(BF16)

    def project(sc_a, sc_b, wkv, wkv_sem):
        scs = [sc_a, sc_b]

        def take_kv(w_ref, i):
            return pltpu.make_async_copy(w_ref.at[pl.ds(i % 2 * HALF, HALF), pl.ds(pl.multiple_of(core * W, W), W)], wkv.at[i], wkv_sem.at[i])

        for i in range(NCH):
            x_in(i).start()
        for i in range(2):
            take_kv(wk_ref, i).start()
        prepare()
        pl.semaphore_wait(barrier, 7)
        for i in range(2, 4):
            take_kv(wv_ref, i).start()
        lax.fori_loop(0, NCH, norm, 0)
        take_queries(0)

        def keys(p):
            part = core if p == 0 else 1 - core
            rows = part_rows(part)
            src = 2 * chip + part
            if p == 0:
                for i in range(2):
                    take_kv(wk_ref, i).wait()
            sc_a[:OWN] = times(rows, wkv.at[0], wkv.at[1])
            if p == 0:
                for i in range(2, 4):
                    take_kv(wv_ref, i).wait()
            sc_a[OWN:] = times(rows, wkv.at[2], wkv.at[3])
            for h in range(KV):
                at = slice(h * HEAD, (h + 1) * HEAD)
                kv[src, 0, h] = turned(sc_a[:OWN, at], rows)
                kv[src, 1, h] = sc_a[OWN:, at].astype(BF16)

            @pl.when(chip == 0)
            def _():
                send(src, 1, p).start()
                send(src, 2, 2 + p).start()

            @pl.when((chip == 1) | (chip == 2))
            def _():
                send(src, 3, p).start()

            if p == 0:
                arrived(0)
            sc_b[rows, :] = times(rows, wbuf.at[0], wbuf.at[1])

        keys(0)
        take_queries(1)
        take_queries(2)
        for i in range(NCH):
            swap(1 - core, i).wait_recv()
        keys(1)
        take_queries(3)

        def epilogue(j):
            for h in range(4):
                q_all[j * 4 + h] = turned(scs[(j + 1) % 2][:, h * HEAD : (h + 1) * HEAD], slice(None))

        for j in range(1, NQ):
            pair = j % 3
            arrived(pair)
            epilogue(j - 1)
            scs[(j + 1) % 2][...] = times(slice(None), wbuf.at[2 * pair], wbuf.at[2 * pair + 1])
            if j + 3 < NQ:
                take_queries(j + 3)
            else:
                for i in range(2):
                    take_out(2 * (j + 3 - NQ) + i, 2 * pair + i).start()
            if j == 2:
                relay(0)
        epilogue(NQ - 1)

    def relay(k):
        @pl.when(chip == 3)
        def _():
            src = 2 + jnp.where(core == k, 0, 1)
            received(src)
            send(src, 2, k).start()

        if k:
            @pl.when((chip == 1) | (chip == 2))
            def _():
                src = chip - 1
                received(src)
                send(src, 3, 2).start()

    pl.run_scoped(project, pltpu.VMEM((TOK, W), F32), pltpu.VMEM((TOK, W), F32), pltpu.VMEM((4, HALF, W), BF16), pltpu.SemaphoreType.DMA((4,)))
    relay(1)

    def attention(top_s, mix_s):
        ones = jnp.ones((8, TOK), BF16)

        def pair_of(b, g):
            k = jnp.concatenate([kv[2 * b, 0, g], kv[2 * b + 1, 0, g]], 0)
            v = jnp.concatenate([kv[2 * b, 1, g], kv[2 * b + 1, 1, g]], 0)
            return k, jnp.concatenate([v.T, ones], 0)

        def own(g, _):
            k, vt = pair_of(chip, g)
            ok = lax.broadcasted_iota(jnp.int32, (OWN, OWN), 0) <= lax.broadcasted_iota(jnp.int32, (OWN, OWN), 1)
            pieces = [(h, part) for h in range(G) for part in range(2)]
            scores = [_dot(k[: (part + 1) * OWN], q_all[g * G + h, part * OWN : (part + 1) * OWN, :], 1, 1) for h, part in pieces]
            weights = []
            for (h, part), s in zip(pieces, scores):
                tri = jnp.where(ok, s[part * OWN :], HIDDEN)
                s = tri if part == 0 else jnp.concatenate([s[:OWN], tri], 0)
                top = s.max(axis=0, keepdims=True)
                top_s[g * G + h, :, part * OWN : (part + 1) * OWN] = top
                weights.append(jnp.exp2((s - top) * SCALE2).astype(BF16))
            for (h, part), p in zip(pieces, weights):
                mix_s[g * G + h, :, part * OWN : (part + 1) * OWN] = _dot(vt[:, : (part + 1) * OWN], p, 1, 0)
            return 0

        lax.fori_loop(0, KV, own, 0)

        def earlier(i, _):
            b = jnp.where(chip == 2, (i - 1), chip - i)

            @pl.when(jnp.logical_not(((chip == 3) & (b == 1)) | ((chip == 1) & (b == 0))))
            def _():
                @pl.when(jnp.logical_not((chip == 2) & (b == 0)))
                def _():
                    received(2 * b + 1)
                received(2 * b)

            @pl.when((chip == 1) & (b == 0))
            def _():
                received(2 * b + 1)

            pieces = [(g, g * G + h, slice(at, at + STRIP)) for g in range(KV) for h in range(G) for at in range(0, TOK, STRIP)]
            pairs = [pair_of(b, g) for g in range(KV)]
            scores, weights = {}, {}
            for i in range(len(pieces) + 2 * AHEAD):
                if i < len(pieces):
                    g, h, at = pieces[i]
                    scores[i] = _dot(pairs[g][0], q_all[h, at, :], 1, 1)
                if 0 <= i - AHEAD < len(pieces):
                    g, h, at = pieces[i - AHEAD]
                    s, old = scores.pop(i - AHEAD), top_s[h, :, at]
                    top = jnp.maximum(old, s.max(axis=0, keepdims=True))
                    top_s[h, :, at] = top
                    weights[i - AHEAD] = jnp.exp2((s - top) * SCALE2).astype(BF16), jnp.exp2((old - top) * SCALE2)
                if 0 <= i - 2 * AHEAD < len(pieces):
                    g, h, at = pieces[i - 2 * AHEAD]
                    p, keep = weights.pop(i - 2 * AHEAD)
                    mix_s[h, :, at] = mix_s[h, :, at] * keep + _dot(pairs[g][1], p, 1, 0)

            return 0

        lax.fori_loop(1, chip + 1, earlier, 0)

        def finish(g, _):
            for h in range(G):
                total = mix_s[g * G + h, HEAD : HEAD + 1, :]
                out = (mix_s[g * G + h, :HEAD, :] * (1 / total)).astype(BF16).T
                o_all[:, pl.ds(pl.multiple_of((g * G + h) * HEAD, HEAD), HEAD)] = out
            return 0

        lax.fori_loop(0, KV, finish, 0)

    for i in range(NCH):
        swap(core, i).wait_send()
    pl.run_scoped(attention, pltpu.VMEM((NH, 1, TOK), F32), pltpu.VMEM((NH, HEAD + 8, TOK), F32))

    def output(yblk, ybuf):
        ring = LAG + 2

        def cross(n):
            slot = lax.rem(n, ring)
            return pltpu.make_async_remote_copy(src_ref=yblk.at[slot, part_rows(1 - core)], dst_ref=yrecv.at[n], send_sem=yss.at[slot],
                                                recv_sem=yrs.at[n], device_id={"sp": partner}, device_id_type=MESH)

        def store(n):
            slot = lax.rem(n, 2)
            return pltpu.make_async_copy(ybuf.at[slot], y_ref.at[:, pl.ds(pl.multiple_of(n * W, W), W)], osem.at[slot])

        def settle(n):
            own = yblk[lax.rem(n, ring), part_rows(core), :]
            res = x_own[:, pl.ds(pl.multiple_of(n * W, W), W)].astype(F32)
            ybuf[lax.rem(n, 2)] = (res + (own + yrecv[n])).astype(BF16)

        def ready(n):
            cross(n).wait()

            @pl.when(n >= 2)
            def _():
                store(n - 2).wait()

        def block(n, settles):
            slot = lax.rem(n, SLOTS)
            take(wo_ref, 0, 0, slot).wait()
            if settles:
                ready(n - LAG)
                settle(n - LAG)
            yblk[lax.rem(n, ring)] = _dot(o_all[...], wbuf[slot], 1, 0)
            cross(n).start()
            if settles:
                store(n - LAG).start()

            @pl.when(n + SLOTS < NOUT)
            def _():
                take_out(n + SLOTS, slot).start()

        for n in range(LAG):
            block(jnp.int32(n), False)
        lax.fori_loop(LAG, NOUT, lambda n, _: (block(n, True), 0)[1], 0)
        for n in range(NOUT - LAG, NOUT):
            ready(jnp.int32(n))
            settle(jnp.int32(n))
            store(jnp.int32(n)).start()
        for n in range(NOUT - 2, NOUT):
            store(jnp.int32(n)).wait()

    pl.run_scoped(output, pltpu.VMEM((LAG + 2, TOK, W), F32), pltpu.VMEM((2, OWN, W), BF16))

    @pl.when(chip == 0)
    def _():
        for k in range(4):
            send(0, 0, k).wait_send()

    @pl.when((chip == 1) | (chip == 2))
    def _():
        for k in range(3):
            send(0, 0, k).wait_send()

    @pl.when(chip == 3)
    def _():
        for k in range(2):
            send(0, 0, k).wait_send()


def solution(mesh):
    def step(x, gain, wq, wk, wv, wo):
        any_, vmem = pl.BlockSpec(memory_space=pl.ANY), pl.BlockSpec(memory_space=pltpu.VMEM)
        dma = pltpu.SemaphoreType.DMA
        return pl.pallas_call(
            _kernel,
            out_shape=jax.ShapeDtypeStruct((OWN, D), BF16),
            in_specs=[any_, vmem, any_, any_, any_, any_],
            out_specs=any_,
            scratch_shapes=[
                pltpu.VMEM((OWN, D), BF16), pltpu.VMEM((TOK, D), BF16), pltpu.VMEM((SLOTS, HALF, W), BF16),
                pltpu.VMEM((2 * CHIPS, 2, KV, OWN, HEAD), BF16), pltpu.VMEM((NH, TOK, HEAD), BF16),
                pltpu.VMEM((NOUT, OWN, W), F32), pltpu.VMEM((TOK, HEAD), F32), pltpu.VMEM((TOK, HEAD), F32), pltpu.VMEM((1, D), F32),
                dma((NCH,)), dma((NCH,)), dma((NCH,)), dma((SLOTS,)), dma((4,)), dma((2 * CHIPS,)), dma((LAG + 2,)), dma((NOUT,)), dma((2,)),
            ],
            compiler_params=pltpu.CompilerParams(collective_id=0, has_side_effects=True, vmem_limit_bytes=67043328),
        )(x, gain.reshape(D // HEAD, HEAD), wq, wk, wv, wo)

    tokens, whole = P(("dp", "sp"), None), P(None, None)
    return jax.shard_map(
        step,
        mesh=mesh,
        in_specs=(tokens, P(None), whole, whole, whole, whole),
        out_specs=tokens,
        check_vma=False,
    )
```

```python
import functools
import math

import jax
import jax.numpy as jnp
from jax import lax
from jax.experimental import pallas as pl
from jax.experimental.pallas import tpu as pltpu
from jax.sharding import PartitionSpec as P

HEAD = 128
THETA = 10000
LOG2E = 1.4426950408889634
HIDDEN = -1e30
MESH = pl.DeviceIdType.MESH
F32, BF16 = jnp.float32, jnp.bfloat16

D = 6144
OWN = 256
TOK = 512
CHIPS = 4
KV = 4
G = 6
NH = KV * G
HALF = D // 2
W = 512
SLOTS = 6
NQ = HALF // W
NOUT = D // W
ROWS = 64
NCH = OWN // ROWS
STRIP = 256
AHEAD = 3
LAG = 2
SCALE2 = HEAD**-0.5 * LOG2E


def _dot(a, b, ca, cb):
    return lax.dot_general(a, b, (((ca,), (cb,)), ((), ())), preferred_element_type=F32)


def _kernel(x_ref, gain_ref, wq_ref, wk_ref, wv_ref, wo_ref, y_ref,
            x_own, a_all, wbuf, kv, q_all, yrecv, cos_s, sin_s, gain_s,
            xsem, as_sem, ar_sem, wsem, kvs, kvr, yss, yrs, osem):
    me = lax.axis_index("sp")
    chip, core = me // 2, me % 2
    partner = me + 1 - 2 * core
    o_all = a_all.at[:, :HALF]

    barrier = pltpu.get_barrier_semaphore()
    for d in range(1, 8):
        pl.semaphore_signal(barrier, inc=1, device_id={"sp": (me + d) % 8}, device_id_type=MESH)

    def take(w_ref, row, col, slot):
        return pltpu.make_async_copy(w_ref.at[pl.ds(row, HALF), pl.ds(col, W)], wbuf.at[slot], wsem.at[slot])

    def take_queries(j):
        col = pl.multiple_of(core * HALF + j * W, W)
        for i in range(2):
            take(wq_ref, i * HALF, col, 2 * (j % 3) + i).start()

    def arrived(pair):
        for i in range(2):
            take(wq_ref, 0, 0, 2 * pair + i).wait()

    def take_out(n, slot):
        return take(wo_ref, pl.multiple_of(core * HALF, HALF), pl.multiple_of(n * W, W), slot)

    def own_rows(i):
        return pl.ds(pl.multiple_of(i * ROWS, ROWS), ROWS)

    def chip_rows(part, i):
        return pl.ds(pl.multiple_of(part * OWN + i * ROWS, ROWS), ROWS)

    def part_rows(part):
        return pl.ds(pl.multiple_of(part * OWN, OWN), OWN)

    def x_in(i):
        return pltpu.make_async_copy(x_ref.at[own_rows(i)], x_own.at[own_rows(i)], xsem.at[i])

    def swap(part, i):
        rows = chip_rows(part, i)
        return pltpu.make_async_remote_copy(src_ref=a_all.at[rows], dst_ref=a_all.at[rows], send_sem=as_sem.at[i], recv_sem=ar_sem.at[i],
                                            device_id={"sp": partner}, device_id_type=MESH)

    def send(src, target, k):
        return pltpu.make_async_remote_copy(src_ref=kv.at[src], dst_ref=kv.at[src], send_sem=kvs.at[k], recv_sem=kvr.at[src],
                                            device_id={"sp": 2 * target + core}, device_id_type=MESH)

    def received(src):
        send(src, 0, 0).wait_recv()

    def prepare():
        gain_s[...] = jnp.concatenate([gain_ref[i : i + 1, :].astype(F32) for i in range(D // HEAD)], 1)
        lane = lax.broadcasted_iota(jnp.int32, (TOK, HEAD), 1)
        place = (chip * TOK + lax.broadcasted_iota(jnp.int32, (TOK, HEAD), 0)).astype(F32)
        angle = place * jnp.exp(lax.rem(lane, HEAD // 2).astype(F32) * (-math.log(THETA) * 2 / HEAD))
        cos_s[...] = jnp.cos(angle)
        sin_s[...] = jnp.where(lane < HEAD // 2, -1.0, 1.0) * jnp.sin(angle)

    def norm(i, _):
        x_in(i).wait()
        total = jnp.zeros((ROWS, HEAD), F32)
        for c in range(D // HEAD):
            wide = x_own[own_rows(i), c * HEAD : (c + 1) * HEAD].astype(F32)
            total += wide * wide
        scale = lax.rsqrt(jnp.sum(total, -1, keepdims=True) * (1 / D) + 1e-6)
        for c in range(D // HEAD):
            at = slice(c * HEAD, (c + 1) * HEAD)
            a_all[chip_rows(core, i), at] = (x_own[own_rows(i), at].astype(F32) * scale * gain_s[:, at]).astype(BF16)
        swap(core, i).start()
        return 0

    def times(rows, low, high):
        return _dot(a_all[rows, :HALF], low[...], 1, 0) + _dot(a_all[rows, HALF:], high[...], 1, 0)

    def turned(t, rows):
        t = t.astype(BF16).astype(F32)
        return (t * cos_s[rows, :] + pltpu.roll(t, HEAD // 2, 1) * sin_s[rows, :]).astype(BF16)

    def start(sc_a, sc_b, wkv, wkv_sem):

        def take_kv(w_ref, i):
            return pltpu.make_async_copy(w_ref.at[pl.ds(i % 2 * HALF, HALF), pl.ds(pl.multiple_of(core * W, W), W)], wkv.at[i], wkv_sem.at[i])

        for i in range(NCH):
            x_in(i).start()
        for i in range(2):
            take_kv(wk_ref, i).start()
        prepare()
        pl.semaphore_wait(barrier, 7)
        for i in range(2, 4):
            take_kv(wv_ref, i).start()
        lax.fori_loop(0, NCH, norm, 0)
        take_queries(0)

        def keys(p, _):
            part = jnp.where(p == 0, core, 1 - core)
            rows = part_rows(part)
            src = 2 * chip + part

            @pl.when(p == 0)
            def _():
                for i in range(2):
                    take_kv(wk_ref, i).wait()

            @pl.when(p == 1)
            def _():
                take_queries(1)
                take_queries(2)
                for i in range(NCH):
                    swap(1 - core, i).wait_recv()

            sc_a[:OWN] = times(rows, wkv.at[0], wkv.at[1])

            @pl.when(p == 0)
            def _():
                for i in range(2, 4):
                    take_kv(wv_ref, i).wait()

            sc_a[OWN:] = times(rows, wkv.at[2], wkv.at[3])
            for h in range(KV):
                at = slice(h * HEAD, (h + 1) * HEAD)
                kv[src, 0, h] = turned(sc_a[:OWN, at], rows)
                kv[src, 1, h] = sc_a[OWN:, at].astype(BF16)

            @pl.when(chip == 0)
            def _():
                send(src, 1, p).start()
                send(src, 2, 2 + p).start()

            @pl.when((chip == 1) | (chip == 2))
            def _():
                send(src, 3, p).start()

            @pl.when(p == 0)
            def _():
                arrived(0)

            sc_b[rows, :] = times(rows, wbuf.at[0], wbuf.at[1])
            return 0

        lax.fori_loop(0, 2, keys, 0)
        take_queries(3)

    def relay(k):
        @pl.when(chip == 3)
        def _():
            src = 2 + jnp.where(core == k, 0, 1)
            received(src)
            send(src, 2, k).start()

        if k:
            @pl.when((chip == 1) | (chip == 2))
            def _():
                src = chip - 1
                received(src)
                send(src, 3, 2).start()

    def pair_of(b, g):
        k = jnp.concatenate([kv[2 * b, 0, g], kv[2 * b + 1, 0, g]], 0)
        v = jnp.concatenate([kv[2 * b, 1, g], kv[2 * b + 1, 1, g]], 0)
        return k, jnp.concatenate([v.T, jnp.ones((8, TOK), BF16)], 0)

    def own(heads, top_s, mix_s, beside=None):
        pairs = {g: pair_of(chip, g) for g in sorted({h // G for h in heads})}
        ok = lax.broadcasted_iota(jnp.int32, (OWN, OWN), 0) <= lax.broadcasted_iota(jnp.int32, (OWN, OWN), 1)
        pieces = [(h, part, slice(part * OWN, (part + 1) * OWN)) for h in heads for part in range(2)]
        scores = [_dot(pairs[h // G][0][: at.stop], q_all[h, at, :], 1, 1) for h, part, at in pieces]
        if beside:
            beside()
        weights = []
        for (h, part, at), s in zip(pieces, scores):
            tri = jnp.where(ok, s[at], HIDDEN)
            s = tri if part == 0 else jnp.concatenate([s[:OWN], tri], 0)
            top = s.max(axis=0, keepdims=True)
            top_s[h, :, at] = top
            weights.append(jnp.exp2((s - top) * SCALE2).astype(BF16))
        for (h, part, at), p in zip(pieces, weights):
            mix_s[h, :, at] = _dot(pairs[h // G][1][:, : at.stop], p, 1, 0)

    def attention(scs, top_s, mix_s):
        def epilogue(j):
            for h in range(4):
                q_all[j * 4 + h] = turned(scs[(j + 1) % 2][:, h * HEAD : (h + 1) * HEAD], slice(None))

        for j in range(1, NQ):
            pair = j % 3
            arrived(pair)

            def times_part(rows):
                scs[(j + 1) % 2][rows, :] = times(rows, wbuf.at[2 * pair], wbuf.at[2 * pair + 1])

            times_part(slice(0, OWN))
            epilogue(j - 1)
            own(range(4 * j - 4, 4 * j), top_s, mix_s, lambda: times_part(slice(OWN, TOK)))
            if j + 3 < NQ:
                take_queries(j + 3)
            else:
                for i in range(2):
                    take_out(2 * (j + 3 - NQ) + i, 2 * pair + i).start()
            if j == 2:
                relay(0)
        epilogue(NQ - 1)
        own(range(4 * NQ - 4, 4 * NQ), top_s, mix_s)
        relay(1)
        for i in range(NCH):
            swap(core, i).wait_send()

        def earlier(i, _):
            b = jnp.where(chip == 2, (i - 1), chip - i)

            @pl.when(jnp.logical_not(((chip == 3) & (b == 1)) | ((chip == 1) & (b == 0))))
            def _():
                @pl.when(jnp.logical_not((chip == 2) & (b == 0)))
                def _():
                    received(2 * b + 1)
                received(2 * b)

            @pl.when((chip == 1) & (b == 0))
            def _():
                received(2 * b + 1)

            pieces = [(g, g * G + h, slice(at, at + STRIP)) for g in range(KV) for h in range(G) for at in range(0, TOK, STRIP)]
            pairs = [pair_of(b, g) for g in range(KV)]
            scores, weights = {}, {}
            for i in range(len(pieces) + 2 * AHEAD):
                if i < len(pieces):
                    g, h, at = pieces[i]
                    scores[i] = _dot(pairs[g][0], q_all[h, at, :], 1, 1)
                if 0 <= i - AHEAD < len(pieces):
                    g, h, at = pieces[i - AHEAD]
                    s, old = scores.pop(i - AHEAD), top_s[h, :, at]
                    top = jnp.maximum(old, s.max(axis=0, keepdims=True))
                    top_s[h, :, at] = top
                    weights[i - AHEAD] = jnp.exp2((s - top) * SCALE2).astype(BF16), jnp.exp2((old - top) * SCALE2)
                if 0 <= i - 2 * AHEAD < len(pieces):
                    g, h, at = pieces[i - 2 * AHEAD]
                    p, keep = weights.pop(i - 2 * AHEAD)
                    mix_s[h, :, at] = mix_s[h, :, at] * keep + _dot(pairs[g][1], p, 1, 0)

            return 0

        lax.fori_loop(1, chip + 1, earlier, 0)

        def finish(g, _):
            for h in range(G):
                total = mix_s[g * G + h, HEAD : HEAD + 1, :]
                out = (mix_s[g * G + h, :HEAD, :] * (1 / total)).astype(BF16).T
                o_all[:, pl.ds(pl.multiple_of((g * G + h) * HEAD, HEAD), HEAD)] = out
            return 0

        lax.fori_loop(0, KV, finish, 0)

    def phase(sc_a, sc_b):
        pl.run_scoped(functools.partial(start, sc_a, sc_b), pltpu.VMEM((4, HALF, W), BF16), pltpu.SemaphoreType.DMA((4,)))
        pl.run_scoped(functools.partial(attention, [sc_a, sc_b]), pltpu.VMEM((NH, 1, TOK), F32), pltpu.VMEM((NH, HEAD + 8, TOK), F32))

    pl.run_scoped(phase, pltpu.VMEM((TOK, W), F32), pltpu.VMEM((TOK, W), F32))

    def output(yblk, ybuf):
        ring = LAG + 2

        def cross(n):
            slot = lax.rem(n, ring)
            return pltpu.make_async_remote_copy(src_ref=yblk.at[slot, part_rows(1 - core)], dst_ref=yrecv.at[n], send_sem=yss.at[slot],
                                                recv_sem=yrs.at[n], device_id={"sp": partner}, device_id_type=MESH)

        def store(n):
            slot = lax.rem(n, 2)
            return pltpu.make_async_copy(ybuf.at[slot], y_ref.at[:, pl.ds(pl.multiple_of(n * W, W), W)], osem.at[slot])

        def settle(n):
            own = yblk[lax.rem(n, ring), part_rows(core), :]
            res = x_own[:, pl.ds(pl.multiple_of(n * W, W), W)].astype(F32)
            ybuf[lax.rem(n, 2)] = (res + (own + yrecv[n])).astype(BF16)

        def ready(n):
            cross(n).wait()

            @pl.when(n >= 2)
            def _():
                store(n - 2).wait()

        def block(n, settles, split=False):
            slot = lax.rem(n, SLOTS)
            take(wo_ref, 0, 0, slot).wait()
            if settles:
                ready(n - LAG)
                settle(n - LAG)
            if split:
                for part in (1 - core, core):
                    rows = part_rows(part)
                    yblk[lax.rem(n, ring), rows, :] = _dot(o_all[rows, :], wbuf[slot], 1, 0)
                    if part is not core:
                        cross(n).start()
            else:
                yblk[lax.rem(n, ring)] = _dot(o_all[...], wbuf[slot], 1, 0)
                cross(n).start()
            if settles:
                store(n - LAG).start()

            @pl.when(n + SLOTS < NOUT)
            def _():
                take_out(n + SLOTS, slot).start()

        for n in range(LAG):
            block(jnp.int32(n), False)
        lax.fori_loop(LAG, NOUT - 1, lambda n, _: (block(n, True), 0)[1], 0)
        block(jnp.int32(NOUT - 1), True, True)
        for n in range(NOUT - LAG, NOUT):
            ready(jnp.int32(n))
            settle(jnp.int32(n))
            store(jnp.int32(n)).start()
        for n in range(NOUT - 2, NOUT):
            store(jnp.int32(n)).wait()

    pl.run_scoped(output, pltpu.VMEM((LAG + 2, TOK, W), F32), pltpu.VMEM((2, OWN, W), BF16))

    @pl.when(chip == 0)
    def _():
        for k in range(4):
            send(0, 0, k).wait_send()

    @pl.when((chip == 1) | (chip == 2))
    def _():
        for k in range(3):
            send(0, 0, k).wait_send()

    @pl.when(chip == 3)
    def _():
        for k in range(2):
            send(0, 0, k).wait_send()


def solution(mesh):
    def step(x, gain, wq, wk, wv, wo):
        any_, vmem = pl.BlockSpec(memory_space=pl.ANY), pl.BlockSpec(memory_space=pltpu.VMEM)
        dma = pltpu.SemaphoreType.DMA
        y = pl.pallas_call(
            _kernel,
            out_shape=jax.ShapeDtypeStruct((OWN, D), BF16),
            in_specs=[any_, vmem, any_, any_, any_, any_],
            out_specs=any_,
            scratch_shapes=[
                pltpu.VMEM((OWN, D), BF16), pltpu.VMEM((TOK, D), BF16), pltpu.VMEM((SLOTS, HALF, W), BF16),
                pltpu.VMEM((2 * CHIPS, 2, KV, OWN, HEAD), BF16), pltpu.VMEM((NH, TOK, HEAD), BF16),
                pltpu.VMEM((NOUT, OWN, W), F32), pltpu.VMEM((TOK, HEAD), F32), pltpu.VMEM((TOK, HEAD), F32), pltpu.VMEM((1, D), F32),
                dma((NCH,)), dma((NCH,)), dma((NCH,)), dma((SLOTS,)), dma((4,)), dma((2 * CHIPS,)), dma((LAG + 2,)), dma((NOUT,)), dma((2,)),
            ],
            compiler_params=pltpu.CompilerParams(collective_id=0, has_side_effects=True, vmem_limit_bytes=67043328),
        )(x, gain.reshape(D // HEAD, HEAD), wq, wk, wv, wo)

        def place(y_ref, out_ref, buf, sem_in, sem_out):
            def at(i):
                return pl.ds(i * ROWS // 2, ROWS // 2)
            ins = [pltpu.make_async_copy(y_ref.at[at(i)], buf.at[at(i)], sem_in.at[i]) for i in range(2 * NCH)]
            outs = [pltpu.make_async_copy(buf.at[at(i)], out_ref.at[at(i)], sem_out.at[i]) for i in range(2 * NCH)]
            for c in ins:
                c.start()
            for i, o in zip(ins, outs):
                i.wait()
                o.start()
            for o in outs:
                o.wait()

        return pl.pallas_call(
            place, out_shape=jax.ShapeDtypeStruct((OWN, D), BF16), in_specs=[any_], out_specs=any_,
            scratch_shapes=[pltpu.VMEM((OWN, D), BF16), dma((2 * NCH,)), dma((2 * NCH,))])(y)

    tokens, whole = P(("dp", "sp"), None), P(None, None)
    return jax.shard_map(
        step,
        mesh=mesh,
        in_specs=(tokens, P(None), whole, whole, whole, whole),
        out_specs=tokens,
        check_vma=False,
    )
```

```python
import functools
import math

import jax
import jax.numpy as jnp
from jax import lax
from jax.experimental import pallas as pl
from jax.experimental.pallas import tpu as pltpu
from jax.sharding import PartitionSpec as P

HEAD = 128
THETA = 10000
LOG2E = 1.4426950408889634
HIDDEN = -1e30
MESH = pl.DeviceIdType.MESH
F32, BF16 = jnp.float32, jnp.bfloat16

D = 6144
OWN = 256
TOK = 512
CHIPS = 4
KV = 4
G = 6
NH = KV * G
HALF = D // 2
W = 512
SLOTS = 6
NQ = HALF // W
NOUT = D // W
ROWS = 64
NCH = OWN // ROWS
STRIP = 256
AHEAD = 3
LAG = 3
SCALE2 = HEAD**-0.5 * LOG2E


def _dot(a, b, ca, cb):
    return lax.dot_general(a, b, (((ca,), (cb,)), ((), ())), preferred_element_type=F32)


def _kernel(x_ref, gain_ref, wq_ref, wk_ref, wv_ref, wo_ref, y_ref,
            x_own, a_all, wbuf, kv, q_all, yrecv, cos_s, sin_s, gain_s,
            xsem, as_sem, ar_sem, wsem, kvs, kvr, yss, yrs, osem):
    me = lax.axis_index("sp")
    chip, core = me // 2, me % 2
    partner = me + 1 - 2 * core
    o_all = a_all.at[:, :HALF]

    barrier = pltpu.get_barrier_semaphore()
    for d in range(1, 8):
        pl.semaphore_signal(barrier, inc=1, device_id={"sp": (me + d) % 8}, device_id_type=MESH)

    def take(w_ref, row, col, slot):
        return pltpu.make_async_copy(w_ref.at[pl.ds(row, HALF), pl.ds(col, W)], wbuf.at[slot], wsem.at[slot])

    def take_queries(j):
        col = pl.multiple_of(core * HALF + j * W, W)
        for i in range(2):
            take(wq_ref, i * HALF, col, 2 * (j % 3) + i).start()

    def arrived(pair):
        for i in range(2):
            take(wq_ref, 0, 0, 2 * pair + i).wait()

    def take_out(n, slot):
        return take(wo_ref, pl.multiple_of(core * HALF, HALF), pl.multiple_of(n * W, W), slot)

    def own_rows(i):
        return pl.ds(pl.multiple_of(i * ROWS, ROWS), ROWS)

    def chip_rows(part, i):
        return pl.ds(pl.multiple_of(part * OWN + i * ROWS, ROWS), ROWS)

    def part_rows(part):
        return pl.ds(pl.multiple_of(part * OWN, OWN), OWN)

    def x_in(i):
        return pltpu.make_async_copy(x_ref.at[own_rows(i)], x_own.at[own_rows(i)], xsem.at[i])

    def swap(part, i):
        rows = chip_rows(part, i)
        return pltpu.make_async_remote_copy(src_ref=a_all.at[rows], dst_ref=a_all.at[rows], send_sem=as_sem.at[i], recv_sem=ar_sem.at[i],
                                            device_id={"sp": partner}, device_id_type=MESH)

    def send(src, target, k):
        return pltpu.make_async_remote_copy(src_ref=kv.at[src], dst_ref=kv.at[src], send_sem=kvs.at[k], recv_sem=kvr.at[src],
                                            device_id={"sp": 2 * target + core}, device_id_type=MESH)

    def received(src):
        send(src, 0, 0).wait_recv()

    def prepare():
        gain_s[...] = jnp.concatenate([gain_ref[i : i + 1, :].astype(F32) for i in range(D // HEAD)], 1)

    def turns():
        lane = lax.broadcasted_iota(jnp.int32, (TOK, HEAD), 1)
        place = (chip * TOK + lax.broadcasted_iota(jnp.int32, (TOK, HEAD), 0)).astype(F32)
        angle = place * jnp.exp(lax.rem(lane, HEAD // 2).astype(F32) * (-math.log(THETA) * 2 / HEAD))
        cos_s[...] = jnp.cos(angle)
        sin_s[...] = jnp.where(lane < HEAD // 2, -1.0, 1.0) * jnp.sin(angle)

    def norm(i, _):
        x_in(i).wait()
        total = jnp.zeros((ROWS, HEAD), F32)
        for c in range(D // HEAD):
            wide = x_own[own_rows(i), c * HEAD : (c + 1) * HEAD].astype(F32)
            total += wide * wide
        scale = lax.rsqrt(jnp.sum(total, -1, keepdims=True) * (1 / D) + 1e-6)
        for c in range(D // HEAD):
            at = slice(c * HEAD, (c + 1) * HEAD)
            a_all[chip_rows(core, i), at] = (x_own[own_rows(i), at].astype(F32) * scale * gain_s[:, at]).astype(BF16)
        swap(core, i).start()
        return 0

    def times(rows, low, high):
        return _dot(a_all[rows, :HALF], low[...], 1, 0) + _dot(a_all[rows, HALF:], high[...], 1, 0)

    def turned(t, rows):
        t = t.astype(BF16).astype(F32)
        return (t * cos_s[rows, :] + pltpu.roll(t, HEAD // 2, 1) * sin_s[rows, :]).astype(BF16)

    def start(sc_a, sc_b, wkv, wkv_sem):

        def take_kv(w_ref, i):
            return pltpu.make_async_copy(w_ref.at[pl.ds(i % 2 * HALF, HALF), pl.ds(pl.multiple_of(core * W, W), W)], wkv.at[i], wkv_sem.at[i])

        for i in range(NCH):
            x_in(i).start()
        for i in range(2):
            take_kv(wk_ref, i).start()
        prepare()
        pl.semaphore_wait(barrier, 7)
        for i in range(2, 4):
            take_kv(wv_ref, i).start()
        lax.fori_loop(0, NCH, norm, 0)
        take_queries(0)
        turns()

        def keys(p, _):
            part = jnp.where(p == 0, core, 1 - core)
            rows = part_rows(part)
            src = 2 * chip + part

            @pl.when(p == 0)
            def _():
                for i in range(2):
                    take_kv(wk_ref, i).wait()

            @pl.when(p == 1)
            def _():
                take_queries(1)
                take_queries(2)
                for i in range(NCH):
                    swap(1 - core, i).wait_recv()

            sc_a[:OWN] = times(rows, wkv.at[0], wkv.at[1])

            @pl.when(p == 0)
            def _():
                for i in range(2, 4):
                    take_kv(wv_ref, i).wait()

            sc_a[OWN:] = times(rows, wkv.at[2], wkv.at[3])
            for h in range(KV):
                at = slice(h * HEAD, (h + 1) * HEAD)
                kv[src, 0, h] = turned(sc_a[:OWN, at], rows)
                kv[src, 1, h] = sc_a[OWN:, at].astype(BF16)

            @pl.when(chip == 0)
            def _():
                send(src, 1, p).start()
                send(src, 2, 2 + p).start()

            @pl.when((chip == 1) | (chip == 2))
            def _():
                send(src, 3, p).start()

            @pl.when(p == 0)
            def _():
                arrived(0)

            sc_b[rows, :] = times(rows, wbuf.at[0], wbuf.at[1])
            return 0

        lax.fori_loop(0, 2, keys, 0)
        take_queries(3)

    def relay(k):
        @pl.when(chip == 3)
        def _():
            src = 2 + jnp.where(core == k, 0, 1)
            received(src)
            send(src, 2, k).start()

        if k:
            @pl.when((chip == 1) | (chip == 2))
            def _():
                src = chip - 1
                received(src)
                send(src, 3, 2).start()

    def pair_of(b, g):
        k = jnp.concatenate([kv[2 * b, 0, g], kv[2 * b + 1, 0, g]], 0)
        v = jnp.concatenate([kv[2 * b, 1, g], kv[2 * b + 1, 1, g]], 0)
        return k, jnp.concatenate([v.T, jnp.ones((8, TOK), BF16)], 0)

    def own(heads, top_s, mix_s, beside=None):
        pairs = {g: pair_of(chip, g) for g in sorted({h // G for h in heads})}
        ok = lax.broadcasted_iota(jnp.int32, (OWN, OWN), 0) <= lax.broadcasted_iota(jnp.int32, (OWN, OWN), 1)
        pieces = [(h, part, slice(part * OWN, (part + 1) * OWN)) for h in heads for part in range(2)]
        scores = [_dot(pairs[h // G][0][: at.stop], q_all[h, at, :], 1, 1) for h, part, at in pieces]
        if beside:
            beside()
        weights = []
        for (h, part, at), s in zip(pieces, scores):
            tri = jnp.where(ok, s[at], HIDDEN)
            s = tri if part == 0 else jnp.concatenate([s[:OWN], tri], 0)
            top = s.max(axis=0, keepdims=True)
            top_s[h, :, at] = top
            weights.append(jnp.exp2((s - top) * SCALE2).astype(BF16))
        for (h, part, at), p in zip(pieces, weights):
            mix_s[h, :, at] = _dot(pairs[h // G][1][:, : at.stop], p, 1, 0)

    def attention(scs, top_s, mix_s):
        def epilogue(j):
            for h in range(4):
                q_all[j * 4 + h] = turned(scs[(j + 1) % 2][:, h * HEAD : (h + 1) * HEAD], slice(None))

        for j in range(1, NQ):
            pair = j % 3
            arrived(pair)

            def times_part(rows):
                scs[(j + 1) % 2][rows, :] = times(rows, wbuf.at[2 * pair], wbuf.at[2 * pair + 1])

            times_part(slice(0, OWN))
            epilogue(j - 1)
            own(range(4 * j - 4, 4 * j), top_s, mix_s, lambda: times_part(slice(OWN, TOK)))
            if j + 3 < NQ:
                take_queries(j + 3)
            else:
                for i in range(2):
                    take_out(2 * (j + 3 - NQ) + i, 2 * pair + i).start()
            if j == 2:
                relay(0)
        epilogue(NQ - 1)
        own(range(4 * NQ - 4, 4 * NQ), top_s, mix_s)
        relay(1)
        for i in range(NCH):
            swap(core, i).wait_send()

        def earlier(i, _):
            b = jnp.where(chip == 2, (i - 1), chip - i)

            @pl.when(jnp.logical_not(((chip == 3) & (b == 1)) | ((chip == 1) & (b == 0))))
            def _():
                @pl.when(jnp.logical_not((chip == 2) & (b == 0)))
                def _():
                    received(2 * b + 1)
                received(2 * b)

            @pl.when((chip == 1) & (b == 0))
            def _():
                received(2 * b + 1)

            pieces = [(g, g * G + h, slice(at, at + STRIP)) for g in range(KV) for h in range(G) for at in range(0, TOK, STRIP)]
            pairs = [pair_of(b, g) for g in range(KV)]
            scores, weights = {}, {}
            for i in range(len(pieces) + 2 * AHEAD):
                if i < len(pieces):
                    g, h, at = pieces[i]
                    scores[i] = _dot(pairs[g][0], q_all[h, at, :], 1, 1)
                if 0 <= i - AHEAD < len(pieces):
                    g, h, at = pieces[i - AHEAD]
                    s, old = scores.pop(i - AHEAD), top_s[h, :, at]
                    top = jnp.maximum(old, s.max(axis=0, keepdims=True))
                    top_s[h, :, at] = top
                    weights[i - AHEAD] = jnp.exp2((s - top) * SCALE2).astype(BF16), jnp.exp2((old - top) * SCALE2)
                if 0 <= i - 2 * AHEAD < len(pieces):
                    g, h, at = pieces[i - 2 * AHEAD]
                    p, keep = weights.pop(i - 2 * AHEAD)
                    mix_s[h, :, at] = mix_s[h, :, at] * keep + _dot(pairs[g][1], p, 1, 0)

            return 0

        lax.fori_loop(1, chip + 1, earlier, 0)

        def finish(g, _):
            for h in range(G):
                total = mix_s[g * G + h, HEAD : HEAD + 1, :]
                out = (mix_s[g * G + h, :HEAD, :] * (1 / total)).astype(BF16).T
                o_all[:, pl.ds(pl.multiple_of((g * G + h) * HEAD, HEAD), HEAD)] = out
            return 0

        lax.fori_loop(0, KV, finish, 0)

    def phase(sc_a, sc_b):
        pl.run_scoped(functools.partial(start, sc_a, sc_b), pltpu.VMEM((4, HALF, W), BF16), pltpu.SemaphoreType.DMA((4,)))
        pl.run_scoped(functools.partial(attention, [sc_a, sc_b]), pltpu.VMEM((NH, 1, TOK), F32), pltpu.VMEM((NH, HEAD + 8, TOK), F32))

    pl.run_scoped(phase, pltpu.VMEM((TOK, W), F32), pltpu.VMEM((TOK, W), F32))

    def output(yblk, ybuf):
        ring = LAG + 2

        def cross(n):
            slot = lax.rem(n, ring)
            return pltpu.make_async_remote_copy(src_ref=yblk.at[slot, part_rows(1 - core)], dst_ref=yrecv.at[n], send_sem=yss.at[slot],
                                                recv_sem=yrs.at[n], device_id={"sp": partner}, device_id_type=MESH)

        def store(n):
            slot = lax.rem(n, 2)
            return pltpu.make_async_copy(ybuf.at[slot], y_ref.at[:, pl.ds(pl.multiple_of(n * W, W), W)], osem.at[slot])

        def settle(n):
            own = yblk[lax.rem(n, ring), part_rows(core), :]
            res = x_own[:, pl.ds(pl.multiple_of(n * W, W), W)].astype(F32)
            ybuf[lax.rem(n, 2)] = (res + (own + yrecv[n])).astype(BF16)

        def ready(n):
            cross(n).wait()

            @pl.when(n >= 2)
            def _():
                store(n - 2).wait()

        def block(n, settles, split=False):
            slot = lax.rem(n, SLOTS)
            take(wo_ref, 0, 0, slot).wait()
            if settles:
                ready(n - LAG)
                settle(n - LAG)
            if split:
                for part in (1 - core, core):
                    rows = part_rows(part)
                    yblk[lax.rem(n, ring), rows, :] = _dot(o_all[rows, :], wbuf[slot], 1, 0)
                    if part is not core:
                        cross(n).start()
            else:
                yblk[lax.rem(n, ring)] = _dot(o_all[...], wbuf[slot], 1, 0)
                cross(n).start()
            if settles:
                store(n - LAG).start()

            @pl.when(n + SLOTS < NOUT)
            def _():
                take_out(n + SLOTS, slot).start()

        for n in range(LAG):
            block(jnp.int32(n), False)
        lax.fori_loop(LAG, NOUT - 1, lambda n, _: (block(n, True), 0)[1], 0)
        block(jnp.int32(NOUT - 1), True, True)
        for n in range(NOUT - LAG, NOUT):
            ready(jnp.int32(n))
            settle(jnp.int32(n))
            store(jnp.int32(n)).start()
        for n in range(NOUT - 2, NOUT):
            store(jnp.int32(n)).wait()

    pl.run_scoped(output, pltpu.VMEM((LAG + 2, TOK, W), F32), pltpu.VMEM((2, OWN, W), BF16))

    @pl.when(chip == 0)
    def _():
        for k in range(4):
            send(0, 0, k).wait_send()

    @pl.when((chip == 1) | (chip == 2))
    def _():
        for k in range(3):
            send(0, 0, k).wait_send()

    @pl.when(chip == 3)
    def _():
        for k in range(2):
            send(0, 0, k).wait_send()


def solution(mesh):
    def step(x, gain, wq, wk, wv, wo):
        any_, vmem = pl.BlockSpec(memory_space=pl.ANY), pl.BlockSpec(memory_space=pltpu.VMEM)
        dma = pltpu.SemaphoreType.DMA
        y = pl.pallas_call(
            _kernel,
            out_shape=jax.ShapeDtypeStruct((OWN, D), BF16),
            in_specs=[any_, vmem, any_, any_, any_, any_],
            out_specs=any_,
            scratch_shapes=[
                pltpu.VMEM((OWN, D), BF16), pltpu.VMEM((TOK, D), BF16), pltpu.VMEM((SLOTS, HALF, W), BF16),
                pltpu.VMEM((2 * CHIPS, 2, KV, OWN, HEAD), BF16), pltpu.VMEM((NH, TOK, HEAD), BF16),
                pltpu.VMEM((NOUT, OWN, W), F32), pltpu.VMEM((TOK, HEAD), F32), pltpu.VMEM((TOK, HEAD), F32), pltpu.VMEM((1, D), F32),
                dma((NCH,)), dma((NCH,)), dma((NCH,)), dma((SLOTS,)), dma((4,)), dma((2 * CHIPS,)), dma((LAG + 2,)), dma((NOUT,)), dma((2,)),
            ],
            compiler_params=pltpu.CompilerParams(collective_id=0, has_side_effects=True, vmem_limit_bytes=67043328),
        )(x, gain.reshape(D // HEAD, HEAD), wq, wk, wv, wo)

        def place(y_ref, out_ref, buf, sem_in, sem_out):
            def at(i):
                return pl.ds(i * ROWS // 2, ROWS // 2)
            ins = [pltpu.make_async_copy(y_ref.at[at(i)], buf.at[at(i)], sem_in.at[i]) for i in range(2 * NCH)]
            outs = [pltpu.make_async_copy(buf.at[at(i)], out_ref.at[at(i)], sem_out.at[i]) for i in range(2 * NCH)]
            for c in ins:
                c.start()
            for i, o in zip(ins, outs):
                i.wait()
                o.start()
            for o in outs:
                o.wait()

        return pl.pallas_call(
            place, out_shape=jax.ShapeDtypeStruct((OWN, D), BF16), in_specs=[any_], out_specs=any_,
            scratch_shapes=[pltpu.VMEM((OWN, D), BF16), dma((2 * NCH,)), dma((2 * NCH,))])(y)

    tokens, whole = P(("dp", "sp"), None), P(None, None)
    return jax.shard_map(
        step,
        mesh=mesh,
        in_specs=(tokens, P(None), whole, whole, whole, whole),
        out_specs=tokens,
        check_vma=False,
    )
```
